256 devices in a mesh: img: 4 (over y, x), rows: 64 (over z, core).
Axes of the slice: x: 2, y: 2, z: 32, core: 2. Of those that a mesh axis runs over, the one named last changes fastest.
The devices are a block of a 4x8x32 slice.
Arguments:
- hidden_states: bfloat16 [3, 32768, 1024], P(None, ('img', 'rows')), parts along dimension 1, may hold values from -6 to 6
- cell_of: int32 [8192], replicated, may hold values from 0 to 8191, as said below
- proj_four_weight: bfloat16 [1024, 256], replicated, may hold values from -0.1875 to 0.1875
- proj_four_bias: float32 [256], replicated, may hold values from -3 to 3
- proj_two_weight: bfloat16 [1024, 512], replicated, may hold values from -0.1875 to 0.1875
- proj_two_bias: float32 [512], replicated, may hold values from -3 to 3
- proj_same_weight: bfloat16 [1024, 1024], replicated, may hold values from -0.1875 to 0.1875
- proj_same_bias: float32 [1024], replicated, may hold values from -3 to 3
- up4_weight: bfloat16 [256, 4096], replicated, may hold values from -0.375 to 0.375
- up4_bias: float32 [256], replicated, may hold values from -3 to 3
- up2_weight: bfloat16 [512, 2048], replicated, may hold values from -0.25 to 0.25
- up2_bias: float32 [512], replicated, may hold values from -3 to 3
- join_weight: bfloat16 [3, 3, 256, 256], replicated, may hold values from -0.125 to 0.125
Outputs:
- joined_four: bfloat16 [2048, 256, 256], P(('img', 'rows')), parts along dimension 0
- upsampled_two: bfloat16 [1024, 128, 512], P(('img', 'rows')), parts along dimension 0
- same_scale: bfloat16 [512, 64, 1024], P(('img', 'rows')), parts along dimension 0
The draws below stay inside these ranges and needn't reach their ends.
There are 4 independent parts, one for each index of `img`. The reference program is written for one: setup_inputs(seed, part) draws one part's arguments, and reference() takes and returns one part's arrays. A program takes and returns all parts, laid end to end along the dimension named above; an argument that names none is the same for every part. Nothing has to cross between parts.
Inputs may be any that keep to these rules, and one draw needn't show every extreme that they name: `cell_of`: a permutation of the cells 0 to 8191; the sequence positions k * 128 to (k + 1) * 128 - 1 hold exactly 2 cells of every block of 128 consecutive cells.
All inputs are finite; a program needn't handle non-finite values.
Results may differ from the reference program's by a relative error of at most 0.0057.
Values may be sent and summed in bfloat16 or wider, within the bound.
A program may use at most 64 MiB of HBM per device.

```python
import jax
import jax.numpy as jnp

HOOKS = 3
HID = 1024
C_FOUR = 256
C_TWO = 512
C_SAME = 1024
FEAT = 256
GRID_W = 64
TOK_DEV = 128
GRID_H = 128
TOKENS = 8192


def draw_cell_of(key, part):
    tile_count = TOKENS // TOK_DEV
    per_tile = TOK_DEV // tile_count
    first_key, second_key = jax.random.split(jax.random.fold_in(key, 11))
    base_cells = jnp.arange(TOKENS, dtype=jnp.int32).reshape(tile_count, TOK_DEV)
    shuffled = jax.random.permutation(first_key, base_cells, axis=1, independent=True)
    dealt = shuffled.reshape(tile_count, tile_count, per_tile).transpose(1, 0, 2).reshape(tile_count, TOK_DEV)
    return jax.random.permutation(second_key, dealt, axis=1, independent=True).reshape(TOKENS)


def levels(own_key, dims, cuts, smallest, largest):
    def one(position, blocks):
        steps = jax.random.uniform(jax.random.fold_in(jax.random.fold_in(own_key, 6), position), (blocks,), jnp.float32, smallest / len(cuts), largest / len(cuts))
        return jnp.repeat(jnp.exp(steps), dims[position] // blocks).reshape((-1,) + (1,) * (len(dims) - position - 1))

    loudness = one(*cuts[0])
    for cut in cuts[1:]:
        loudness = loudness * one(*cut)
    return loudness


def bell_draw(own_key, shape, spread, most, cuts=(), kind=jnp.bfloat16):
    values = spread * jax.random.normal(own_key, shape, jnp.float32)
    if cuts:
        values = values * levels(own_key, shape, cuts, -0.22, 0.18)
    return jnp.clip(values, -most, most).astype(kind)


def setup_inputs(seed: int = 0, part: int = 0) -> dict:
    splits = jax.random.split(jax.random.key(seed), 14)
    part_keys = jax.random.split(jax.random.fold_in(splits[13], part), 14)
    return {
        "hidden_states": bell_draw(part_keys[0], (HOOKS, TOKENS, HID), 1.0, 6.0, ((1, 64),)),
        "cell_of": draw_cell_of(jax.random.fold_in(splits[13], 71), part),
        "proj_four_weight": bell_draw(splits[2], (HID, C_FOUR), HID ** -0.5, 0.1875),
        "proj_four_bias": bell_draw(splits[3], (C_FOUR,), 0.5, 3.0, (), jnp.float32),
        "proj_two_weight": bell_draw(splits[4], (HID, C_TWO), HID ** -0.5, 0.1875),
        "proj_two_bias": bell_draw(splits[5], (C_TWO,), 0.5, 3.0, (), jnp.float32),
        "proj_same_weight": bell_draw(splits[6], (HID, C_SAME), HID ** -0.5, 0.1875),
        "proj_same_bias": bell_draw(splits[7], (C_SAME,), 0.5, 3.0, (), jnp.float32),
        "up4_weight": bell_draw(splits[8], (C_FOUR, 16 * C_FOUR), C_FOUR ** -0.5, 0.375),
        "up4_bias": bell_draw(splits[9], (C_FOUR,), 0.5, 3.0, (), jnp.float32),
        "up2_weight": bell_draw(splits[10], (C_TWO, 4 * C_TWO), C_TWO ** -0.5, 0.25),
        "up2_bias": bell_draw(splits[11], (C_TWO,), 0.5, 3.0, (), jnp.float32),
        "join_weight": bell_draw(splits[12], (3, 3, C_FOUR, FEAT), (9 * C_FOUR) ** -0.5, 0.125),
    }


def expand(proj, weight, bias_row, factor):
    height, columns, channels = proj.shape
    out_channels = weight.shape[1] // (factor * factor)
    flattened = jnp.dot(proj.reshape(-1, channels), weight, preferred_element_type=jnp.float32)
    flattened = flattened + jnp.tile(bias_row, factor * factor)[None, :]
    result = flattened.astype(jnp.bfloat16).reshape(height, columns, factor, factor, out_channels)
    return result.transpose(0, 2, 1, 3, 4).reshape(height * factor, columns * factor, out_channels)


def convolve(padded, weight, out_rows, out_cols):
    channels = padded.shape[2]
    total = jnp.zeros((out_rows, out_cols, weight.shape[3]), jnp.float32)
    for row_tap in range(3):
        for col_tap in range(3):
            window = padded[row_tap:row_tap + out_rows, col_tap:col_tap + out_cols]
            term = jnp.dot(window.reshape(-1, channels), weight[row_tap, col_tap], preferred_element_type=jnp.float32)
            total = total + term.reshape(out_rows, out_cols, -1)
    return total.astype(jnp.bfloat16)


def reference(hidden_states, cell_of, proj_four_weight, proj_four_bias, proj_two_weight, proj_two_bias, proj_same_weight, proj_same_bias, up4_weight, up4_bias, up2_weight, up2_bias, join_weight):
    grid_tokens = jnp.zeros(hidden_states.shape, jnp.bfloat16).at[:, cell_of, :].set(hidden_states)
    pairs = ((proj_four_weight, proj_four_bias), (proj_two_weight, proj_two_bias), (proj_same_weight, proj_same_bias))
    maps = []
    for hook in range(HOOKS):
        projected = jnp.dot(grid_tokens[hook], pairs[hook][0], preferred_element_type=jnp.float32) + pairs[hook][1]
        maps.append(projected.astype(jnp.bfloat16).reshape(GRID_H, GRID_W, -1))
    upsampled_four = expand(maps[0], up4_weight, up4_bias, 4)
    padded = jnp.pad(upsampled_four, ((1, 1), (1, 1), (0, 0)))
    joined_four = convolve(padded, join_weight, 4 * GRID_H, 4 * GRID_W)
    upsampled_two = expand(maps[1], up2_weight, up2_bias, 2)
    same_scale = maps[2]
    return (joined_four, upsampled_two, same_scale)
```

```python
import functools

import jax
import jax.numpy as jnp
from jax import lax
from jax.experimental import pallas as pl
from jax.experimental.pallas import tpu as pltpu
from jax.sharding import PartitionSpec as P

GRID_W = 64
F32 = jnp.float32
BF16 = jnp.bfloat16


def dot(a, b):
    return jnp.dot(a, b, preferred_element_type=F32)


def dot_first(a, b):
    return lax.dot_general(a, b, (((0,), (0,)), ((), ())), preferred_element_type=F32)


def iota(shape, dim):
    return lax.broadcasted_iota(jnp.int32, shape, dim)


def one_hot(mask):
    return jnp.where(mask, 1.0, 0.0).astype(BF16)


def kernel(
    shards,
    hidden_hbm,
    cells_hbm,
    w4_hbm,
    b4_hbm,
    w2_hbm,
    b2_hbm,
    w1_hbm,
    b1_hbm,
    u4_hbm,
    c4_hbm,
    u2_hbm,
    c2_hbm,
    join_hbm,
    joined_hbm,
    up2_hbm,
    same_hbm,
    hidden,
    cells,
    w4,
    b4,
    w2,
    b2,
    w1,
    b1,
    u4,
    c4,
    u2,
    c2,
    join,
    in4,
    in2,
    in1,
    send4,
    send2,
    send1,
    edge,
    rim,
    phases,
    mixed,
    joined,
    wide,
    same,
    load_sem,
    send_sem,
    recv_sem,
    edge_send,
    edge_recv,
    store_sem,
):
    me = lax.axis_index("rows")
    tile = hidden.shape[1]
    half = tile // 2

    def remote(src, dst, send, recv, peer):
        return pltpu.make_async_remote_copy(
            src_ref=src,
            dst_ref=dst,
            send_sem=send,
            recv_sem=recv,
            device_id={"rows": peer},
            device_id_type=pl.DeviceIdType.MESH,
        )

    loads = [
        pltpu.make_async_copy(src, dst, load_sem.at[k])
        for k, (src, dst) in enumerate(
            [
                (cells_hbm, cells),
                (hidden_hbm.at[0], hidden.at[0]),
                (w4_hbm, w4),
                (b4_hbm, b4),
                (hidden_hbm.at[1], hidden.at[1]),
                (w2_hbm, w2),
                (b2_hbm, b2),
                (hidden_hbm.at[2], hidden.at[2]),
                (w1_hbm, w1),
                (b1_hbm, b1),
                (u4_hbm, u4),
                (c4_hbm, c4),
                (join_hbm, join),
                (u2_hbm, u2),
                (c2_hbm, c2),
            ]
        )
    ]
    for load in loads:
        load.start()

    barrier = pltpu.get_barrier_semaphore()

    @pl.loop(1, shards)
    def _(k):
        pl.semaphore_signal(
            barrier,
            inc=1,
            device_id={"rows": lax.rem(me + k, shards)},
            device_id_type=pl.DeviceIdType.MESH,
        )

    loads[0].wait()
    mine = cells[pl.ds(me, 1), :]
    row = iota((tile, tile), 0)
    owner = lax.div(mine, tile) == lax.div(row, 2)
    low = jnp.min(jnp.where(owner, mine, shards * tile), axis=1, keepdims=True)
    outgoing = one_hot(owner & ((mine == low) == (lax.rem(row, 2) == 0)))

    table = cells[...]
    here = lax.div(table, tile) == me
    local = lax.rem(table, tile)
    first = jnp.min(jnp.where(here, local, tile), axis=1, keepdims=True)
    last = jnp.max(jnp.where(here, local, -1), axis=1, keepdims=True)
    twice = one_hot(lax.div(iota((tile, shards), 0), 2) == iota((tile, shards), 1))
    wide_first = dot(twice, jnp.broadcast_to(first, (shards, tile)).astype(F32).astype(BF16))
    wide_last = dot(twice, jnp.broadcast_to(last, (shards, tile)).astype(F32).astype(BF16))
    target = jnp.where(lax.rem(row, 2) == 0, wide_first, wide_last)
    placing = one_hot(target == iota((tile, tile), 1).astype(F32))

    def project(layer, weight, bias):
        value = dot(hidden[layer], weight[...]) + bias[...]
        return dot(outgoing, value.astype(BF16)).astype(BF16)

    sends = (send4, send2, send1)
    arrivals = (in4, in2, in1)

    def put(piece, value):
        sends[piece][...] = value.reshape(shards, 2, value.shape[1])

    def launch(piece):
        @pl.loop(1, shards)
        def _(k):
            peer = lax.rem(me + k, shards)
            remote(
                sends[piece].at[peer],
                arrivals[piece].at[me],
                send_sem.at[piece],
                recv_sem.at[piece],
                peer,
            ).start()

        pltpu.make_async_copy(
            sends[piece].at[me], arrivals[piece].at[me], recv_sem.at[piece]
        ).start()

    for k in (1, 2, 3):
        loads[k].wait()
    put(0, project(0, w4, b4))
    for k in (4, 5, 6):
        loads[k].wait()
    put(1, project(1, w2, b2))
    pl.semaphore_wait(barrier, shards - 1)
    launch(0)
    launch(1)
    for k in (7, 8, 9):
        loads[k].wait()
    put(2, project(2, w1, b1))
    launch(2)

    def collect(piece):
        buffer = arrivals[piece]
        pltpu.make_async_copy(buffer, buffer, recv_sem.at[piece]).wait()
        value = buffer[...].reshape(tile, buffer.shape[2])
        return dot_first(placing, value).astype(BF16)

    tile4 = collect(0)
    edge[...] = tile4
    upper, lower = lax.max(me - 1, 0), lax.min(me + 1, shards - 1)
    to_upper = remote(
        edge.at[pl.ds(0, half)], rim.at[1], edge_send.at[0], edge_recv.at[1], upper
    )
    to_lower = remote(
        edge.at[pl.ds(half, half)], rim.at[0], edge_send.at[1], edge_recv.at[0], lower
    )

    @pl.when(me > 0)
    def _():
        to_upper.start()

    @pl.when(me < shards - 1)
    def _():
        to_lower.start()

    for k in (10, 11, 12):
        loads[k].wait()
    feat = c4.shape[1]
    column = lax.rem(iota((tile, feat), 0), half)

    def spread(value, phase, place):
        place(phase + 1, value)
        if phase == 3:
            rolled = pltpu.roll(value, 1, 0)
            place(0, jnp.where(column[: value.shape[0]] == 0, 0.0, rolled))
        if phase == 0:
            rolled = pltpu.roll(value, value.shape[0] - 1, 0)
            place(5, jnp.where(column[: value.shape[0]] == half - 1, 0.0, rolled))

    for a in range(4):
        for b in range(4):
            at = (a * 4 + b) * feat
            value = dot(tile4, u4[:, at : at + feat]) + c4[...]

            def place(slot, rows, a=a):
                rows = rows.astype(BF16)
                phases[slot, pl.ds((1 + a) * half, half), :] = rows[:half]
                phases[slot, pl.ds((5 + a) * half, half), :] = rows[half:]

            spread(value, b, place)

    @pl.when(me > 0)
    def _():
        to_upper.wait_send()
        to_lower.wait_recv()

    @pl.when(me < shards - 1)
    def _():
        to_lower.wait_send()
        to_upper.wait_recv()

    for side, a, keep, at_row in ((0, 3, me > 0, 0), (1, 0, me < shards - 1, 9)):

        @pl.when(keep)
        def _():
            for b in range(4):
                at = (a * 4 + b) * feat
                value = dot(rim[side], u4[:, at : at + feat]) + c4[...]

                def place(slot, rows):
                    phases[slot, pl.ds(at_row * half, half), :] = rows.astype(BF16)

                spread(value, b, place)

        @pl.when(jnp.logical_not(keep))
        def _():
            for slot in range(6):
                phases[slot, pl.ds(at_row * half, half), :] = jnp.zeros((half, feat), BF16)

    @pl.loop(0, 4)
    def _(phase):
        taps = []
        for a in range(3):
            for b in range(3):
                taps.append(phases[phase + b, pl.ds(a * half, 8 * half), :])
        value = dot(jnp.concatenate(taps, axis=1), join[...])
        mixed[phase] = value.astype(BF16).reshape(8, half, value.shape[1])

    order = iota((4 * half, 4 * half), 0)
    source = iota((4 * half, 4 * half), 1)
    weave4 = one_hot(source == lax.rem(order, 4) * half + lax.div(order, 4))

    @pl.loop(0, 8)
    def _(r):
        columns = mixed[:, r].reshape(4 * half, mixed.shape[3])
        joined[r] = dot(weave4, columns).astype(BF16)
        pltpu.make_async_copy(joined.at[r], joined_hbm.at[r], store_sem.at[0]).start()

    tile2 = collect(1)
    for k in (13, 14):
        loads[k].wait()
    weave2 = one_hot(
        iota((tile, tile), 1) == lax.rem(row, 2) * half + lax.div(row, 2)
    )
    c_two = c2.shape[1]
    for a in range(2):
        pair = [
            (dot(tile2, u2[:, at : at + c_two]) + c2[...]).astype(BF16)
            for at in ((a * 2) * c_two, (a * 2 + 1) * c_two)
        ]
        for i in range(2):
            both = jnp.concatenate([p[i * half : (i + 1) * half] for p in pair], axis=0)
            wide[2 * i + a] = dot(weave2, both).astype(BF16)
    pltpu.make_async_copy(wide, up2_hbm, store_sem.at[1]).start()

    tile1 = collect(2)
    same[...] = tile1.reshape(2, half, tile1.shape[1])
    pltpu.make_async_copy(same, same_hbm, store_sem.at[2]).start()

    for piece in range(3):
        most = sends[piece].at[pl.ds(0, shards - 1)]
        pltpu.make_async_copy(most, most, send_sem.at[piece]).wait()
    pltpu.make_async_copy(joined, joined_hbm, store_sem.at[0]).wait()
    pltpu.make_async_copy(wide, up2_hbm, store_sem.at[1]).wait()
    pltpu.make_async_copy(same, same_hbm, store_sem.at[2]).wait()


def body(
    hidden_states,
    cell_of,
    proj_four_weight,
    proj_four_bias,
    proj_two_weight,
    proj_two_bias,
    proj_same_weight,
    proj_same_bias,
    up4_weight,
    up4_bias,
    up2_weight,
    up2_bias,
    join_weight,
):
    shards = lax.axis_size("rows")
    tile = hidden_states.shape[1]
    half = tile // 2
    four, two, one = (
        proj_four_weight.shape[1],
        proj_two_weight.shape[1],
        proj_same_weight.shape[1],
    )
    feat = join_weight.shape[3]
    operands = (
        hidden_states,
        cell_of.reshape(shards, tile),
        proj_four_weight,
        proj_four_bias.reshape(1, -1),
        proj_two_weight,
        proj_two_bias.reshape(1, -1),
        proj_same_weight,
        proj_same_bias.reshape(1, -1),
        up4_weight,
        up4_bias.reshape(1, -1),
        up2_weight,
        up2_bias.reshape(1, -1),
        join_weight.reshape(-1, feat),
    )
    vmem = pltpu.VMEM
    return tuple(
        pl.pallas_call(
            functools.partial(kernel, shards),
            out_shape=(
                jax.ShapeDtypeStruct((8, 4 * half, feat), BF16),
                jax.ShapeDtypeStruct((4, 2 * half, two), BF16),
                jax.ShapeDtypeStruct((2, half, one), BF16),
            ),
            in_specs=[pl.BlockSpec(memory_space=pltpu.HBM)] * len(operands),
            out_specs=[pl.BlockSpec(memory_space=pltpu.HBM)] * 3,
            scratch_shapes=[vmem(o.shape, o.dtype) for o in operands]
            + [
                vmem((shards, 2, four), BF16),
                vmem((shards, 2, two), BF16),
                vmem((shards, 2, one), BF16),
                vmem((shards, 2, four), BF16),
                vmem((shards, 2, two), BF16),
                vmem((shards, 2, one), BF16),
                vmem((tile, four), BF16),
                vmem((2, half, four), BF16),
                vmem((6, 10 * half, four), BF16),
                vmem((4, 8, half, feat), BF16),
                vmem((8, 4 * half, feat), BF16),
                vmem((4, 2 * half, two), BF16),
                vmem((2, half, one), BF16),
                pltpu.SemaphoreType.DMA((15,)),
                pltpu.SemaphoreType.DMA((3,)),
                pltpu.SemaphoreType.DMA((3,)),
                pltpu.SemaphoreType.DMA((2,)),
                pltpu.SemaphoreType.DMA((2,)),
                pltpu.SemaphoreType.DMA((3,)),
            ],
            compiler_params=pltpu.CompilerParams(
                collective_id=0, has_side_effects=True, vmem_limit_bytes=66_000_000
            ),
            name="pyramid",
        )(*operands)
    )


def solution(mesh):
    rows = P(("img", "rows"), None, None)
    return jax.shard_map(
        body,
        mesh=mesh,
        in_specs=(P(None, ("img", "rows"), None),) + (P(),) * 12,
        out_specs=(rows,) * 3,
        check_vma=False,
    )
```

```python
import functools

import jax
import jax.numpy as jnp
from jax import lax
from jax.experimental import pallas as pl
from jax.experimental.pallas import tpu as pltpu
from jax.sharding import PartitionSpec as P

GRID_W = 64
NEAR = 4
F32 = jnp.float32
BF16 = jnp.bfloat16


def dot(a, b):
    return jnp.dot(a, b, preferred_element_type=F32)


def dot_first(a, b):
    return lax.dot_general(a, b, (((0,), (0,)), ((), ())), preferred_element_type=F32)


def iota(shape, dim):
    return lax.broadcasted_iota(jnp.int32, shape, dim)


def one_hot(mask):
    return jnp.where(mask, 1.0, 0.0).astype(BF16)


def kernel(
    shards,
    hidden_hbm,
    cells_hbm,
    w4_hbm,
    b4_hbm,
    w2_hbm,
    b2_hbm,
    w1_hbm,
    b1_hbm,
    u4_hbm,
    c4_hbm,
    u2_hbm,
    c2_hbm,
    join_hbm,
    joined_hbm,
    up2_hbm,
    same_hbm,
    hidden,
    cells,
    w4,
    b4,
    w2,
    b2,
    w1,
    b1,
    u4,
    c4,
    u2,
    c2,
    join,
    in4,
    in2,
    in1,
    send4,
    send2,
    send1,
    edge,
    rim,
    phases,
    mixed,
    joined,
    wide,
    same,
    load_sem,
    send_sem,
    recv_sem,
    edge_send,
    edge_recv,
    store_sem,
    known_sem,
):
    me = lax.axis_index("rows")
    tile = hidden.shape[1]
    half = tile // 2

    def remote(src, dst, send, recv, peer):
        return pltpu.make_async_remote_copy(
            src_ref=src,
            dst_ref=dst,
            send_sem=send,
            recv_sem=recv,
            device_id={"rows": peer},
            device_id_type=pl.DeviceIdType.MESH,
        )

    loads = [
        pltpu.make_async_copy(src, dst, load_sem.at[k])
        for k, (src, dst) in enumerate(
            [
                (cells_hbm, cells),
                (hidden_hbm.at[0], hidden.at[0]),
                (w4_hbm, w4),
                (b4_hbm, b4),
                (hidden_hbm.at[1], hidden.at[1]),
                (w2_hbm, w2),
                (b2_hbm, b2),
                (hidden_hbm.at[2], hidden.at[2]),
                (w1_hbm, w1),
                (b1_hbm, b1),
                (u4_hbm, u4),
                (c4_hbm, c4),
                (join_hbm, join),
                (u2_hbm, u2),
                (c2_hbm, c2),
            ]
        )
    ]
    for load in loads:
        load.start()

    barrier = pltpu.get_barrier_semaphore()
    chips = shards // 2
    z = lax.div(me, 2)
    core = lax.rem(me, 2)
    rounds = chips // 2 // NEAR

    def signal(sem, peer):
        pl.semaphore_signal(
            sem, inc=1, device_id={"rows": peer}, device_id_type=pl.DeviceIdType.MESH
        )

    def around(d):
        return lax.rem(z + d + chips, chips)

    signal(barrier, me + 1 - 2 * core)

    @pl.loop(1, NEAR + 1)
    def _(d):
        for side in (d, -d):
            for other in range(2):
                signal(barrier, 2 * around(side) + other)

    def known(k):
        if k == 0:
            pl.semaphore_wait(barrier, 4 * NEAR + 1)
        else:
            pl.semaphore_wait(known_sem.at[2 * k - 2], 1)
            pl.semaphore_wait(known_sem.at[2 * k - 1], 1)
        if k < rounds - 1:
            signal(known_sem.at[2 * k], 2 * around(NEAR) + core)
            signal(known_sem.at[2 * k + 1], 2 * around(-NEAR) + core)

    loads[0].wait()
    mine = cells[pl.ds(me, 1), :]
    row = iota((tile, tile), 0)
    owner = lax.div(mine, tile) == lax.div(row, 2)
    low = jnp.min(jnp.where(owner, mine, shards * tile), axis=1, keepdims=True)
    outgoing = one_hot(owner & ((mine == low) == (lax.rem(row, 2) == 0)))

    table = cells[...]
    here = lax.div(table, tile) == me
    local = lax.rem(table, tile)
    first = jnp.min(jnp.where(here, local, tile), axis=1, keepdims=True)
    final = jnp.max(jnp.where(here, local, -1), axis=1, keepdims=True)
    twice = one_hot(lax.div(iota((tile, shards), 0), 2) == iota((tile, shards), 1))
    wide_first = dot(twice, jnp.broadcast_to(first, (shards, tile)).astype(F32).astype(BF16))
    wide_last = dot(twice, jnp.broadcast_to(final, (shards, tile)).astype(F32).astype(BF16))
    target = jnp.where(lax.rem(row, 2) == 0, wide_first, wide_last)
    placing = one_hot(target == iota((tile, tile), 1).astype(F32))

    def project(layer, weight, bias):
        value = dot(hidden[layer], weight[...]) + bias[...]
        return dot(outgoing, value.astype(BF16)).astype(BF16)

    sends = (send4, send2, send1)
    arrivals = (in4, in2, in1)

    def put(piece, value):
        sends[piece][...] = value.reshape(shards, 2, value.shape[1])

    def fling(pieces, chip):
        for other in range(2):
            for piece in pieces:
                remote(
                    sends[piece].at[2 * chip + other],
                    arrivals[piece].at[me],
                    send_sem.at[piece],
                    recv_sem.at[piece],
                    2 * chip + other,
                ).start()

    def home(piece):
        pltpu.make_async_copy(
            sends[piece].at[me], arrivals[piece].at[me], recv_sem.at[piece]
        ).start()
        peer = me + 1 - 2 * core
        remote(
            sends[piece].at[peer],
            arrivals[piece].at[me],
            send_sem.at[piece],
            recv_sem.at[piece],
            peer,
        ).start()

    def spanning(pieces, low, high, down=True):
        @pl.loop(0, high - low + 1)
        def _(k):
            d = high - k if down else low + k
            fling(pieces, around(d))

            @pl.when(d < chips // 2)
            def _():
                fling(pieces, around(-d))

    for k in (1, 2, 3):
        loads[k].wait()
    put(0, project(0, w4, b4))
    for k in (4, 5, 6):
        loads[k].wait()
    put(1, project(1, w2, b2))
    for k in (7, 8, 9):
        loads[k].wait()
    put(2, project(2, w1, b1))
    known(0)
    spanning((0, 1, 2), 1, 4)
    known(1)
    spanning((0, 1), 5, 8)
    known(2)
    spanning((0, 1), 9, 12)
    known(3)
    spanning((0,), 13, 16)
    spanning((1, 2), 13, 16)
    for piece in range(3):
        home(piece)

    def collect(piece):
        buffer = arrivals[piece]
        pltpu.make_async_copy(buffer, buffer, recv_sem.at[piece]).wait()
        value = buffer[...].reshape(tile, buffer.shape[2])
        return dot_first(placing, value).astype(BF16)

    tile4 = collect(0)
    edge[...] = tile4
    upper, lower = lax.max(me - 1, 0), lax.min(me + 1, shards - 1)
    to_upper = remote(
        edge.at[pl.ds(0, half)], rim.at[1], edge_send.at[0], edge_recv.at[1], upper
    )
    to_lower = remote(
        edge.at[pl.ds(half, half)], rim.at[0], edge_send.at[1], edge_recv.at[0], lower
    )

    @pl.when(me > 0)
    def _():
        to_upper.start()

    @pl.when(me < shards - 1)
    def _():
        to_lower.start()

    spanning((2,), 5, 12)
    for k in (10, 11, 12):
        loads[k].wait()
    feat = c4.shape[1]
    column = lax.rem(iota((tile, feat), 0), half)

    def spread(value, phase, place):
        place(phase + 1, value)
        if phase == 3:
            rolled = pltpu.roll(value, 1, 0)
            place(0, jnp.where(column[: value.shape[0]] == 0, 0.0, rolled))
        if phase == 0:
            rolled = pltpu.roll(value, value.shape[0] - 1, 0)
            place(5, jnp.where(column[: value.shape[0]] == half - 1, 0.0, rolled))

    for a in range(4):
        for b in range(4):
            at = (a * 4 + b) * feat
            value = dot(tile4, u4[:, at : at + feat]) + c4[...]

            def place(slot, rows, a=a):
                rows = rows.astype(BF16)
                phases[slot, pl.ds((1 + a) * half, half), :] = rows[:half]
                phases[slot, pl.ds((5 + a) * half, half), :] = rows[half:]

            spread(value, b, place)

    @pl.when(me > 0)
    def _():
        to_upper.wait_send()
        to_lower.wait_recv()

    @pl.when(me < shards - 1)
    def _():
        to_lower.wait_send()
        to_upper.wait_recv()

    for side, a, keep, at_row in ((0, 3, me > 0, 0), (1, 0, me < shards - 1, 9)):

        @pl.when(keep)
        def _():
            for b in range(4):
                at = (a * 4 + b) * feat
                value = dot(rim[side], u4[:, at : at + feat]) + c4[...]

                def place(slot, rows):
                    phases[slot, pl.ds(at_row * half, half), :] = rows.astype(BF16)

                spread(value, b, place)

        @pl.when(jnp.logical_not(keep))
        def _():
            for slot in range(6):
                phases[slot, pl.ds(at_row * half, half), :] = jnp.zeros((half, feat), BF16)

    @pl.loop(0, 4)
    def _(phase):
        taps = []
        for a in range(3):
            for b in range(3):
                taps.append(phases[phase + b, pl.ds(a * half, 8 * half), :])
        value = dot(jnp.concatenate(taps, axis=1), join[...])
        mixed[phase] = value.astype(BF16).reshape(8, half, value.shape[1])

    order = iota((4 * half, 4 * half), 0)
    source = iota((4 * half, 4 * half), 1)
    weave4 = one_hot(source == lax.rem(order, 4) * half + lax.div(order, 4))

    @pl.loop(0, 8)
    def _(r):
        columns = mixed[:, r].reshape(4 * half, mixed.shape[3])
        joined[r] = dot(weave4, columns).astype(BF16)
        pltpu.make_async_copy(joined.at[r], joined_hbm.at[r], store_sem.at[0]).start()

    tile2 = collect(1)
    for k in (13, 14):
        loads[k].wait()
    weave2 = one_hot(
        iota((tile, tile), 1) == lax.rem(row, 2) * half + lax.div(row, 2)
    )
    c_two = c2.shape[1]
    for a in range(2):
        pair = [
            (dot(tile2, u2[:, at : at + c_two]) + c2[...]).astype(BF16)
            for at in ((a * 2) * c_two, (a * 2 + 1) * c_two)
        ]
        for i in range(2):
            both = jnp.concatenate([p[i * half : (i + 1) * half] for p in pair], axis=0)
            wide[2 * i + a] = dot(weave2, both).astype(BF16)
    pltpu.make_async_copy(wide, up2_hbm, store_sem.at[1]).start()

    tile1 = collect(2)
    same[...] = tile1.reshape(2, half, tile1.shape[1])
    pltpu.make_async_copy(same, same_hbm, store_sem.at[2]).start()

    for piece in range(3):
        most = sends[piece].at[pl.ds(0, shards - 1)]
        pltpu.make_async_copy(most, most, send_sem.at[piece]).wait()
    pltpu.make_async_copy(joined, joined_hbm, store_sem.at[0]).wait()
    pltpu.make_async_copy(wide, up2_hbm, store_sem.at[1]).wait()
    pltpu.make_async_copy(same, same_hbm, store_sem.at[2]).wait()


def body(
    hidden_states,
    cell_of,
    proj_four_weight,
    proj_four_bias,
    proj_two_weight,
    proj_two_bias,
    proj_same_weight,
    proj_same_bias,
    up4_weight,
    up4_bias,
    up2_weight,
    up2_bias,
    join_weight,
):
    shards = lax.axis_size("rows")
    tile = hidden_states.shape[1]
    half = tile // 2
    four, two, one = (
        proj_four_weight.shape[1],
        proj_two_weight.shape[1],
        proj_same_weight.shape[1],
    )
    feat = join_weight.shape[3]
    operands = (
        hidden_states,
        cell_of.reshape(shards, tile),
        proj_four_weight,
        proj_four_bias.reshape(1, -1),
        proj_two_weight,
        proj_two_bias.reshape(1, -1),
        proj_same_weight,
        proj_same_bias.reshape(1, -1),
        up4_weight,
        up4_bias.reshape(1, -1),
        up2_weight,
        up2_bias.reshape(1, -1),
        join_weight.reshape(-1, feat),
    )
    vmem = pltpu.VMEM
    return tuple(
        pl.pallas_call(
            functools.partial(kernel, shards),
            out_shape=(
                jax.ShapeDtypeStruct((8, 4 * half, feat), BF16),
                jax.ShapeDtypeStruct((4, 2 * half, two), BF16),
                jax.ShapeDtypeStruct((2, half, one), BF16),
            ),
            in_specs=[pl.BlockSpec(memory_space=pltpu.HBM)] * len(operands),
            out_specs=[pl.BlockSpec(memory_space=pltpu.HBM)] * 3,
            scratch_shapes=[vmem(o.shape, o.dtype) for o in operands]
            + [
                vmem((shards, 2, four), BF16),
                vmem((shards, 2, two), BF16),
                vmem((shards, 2, one), BF16),
                vmem((shards, 2, four), BF16),
                vmem((shards, 2, two), BF16),
                vmem((shards, 2, one), BF16),
                vmem((tile, four), BF16),
                vmem((2, half, four), BF16),
                vmem((6, 10 * half, four), BF16),
                vmem((4, 8, half, feat), BF16),
                vmem((8, 4 * half, feat), BF16),
                vmem((4, 2 * half, two), BF16),
                vmem((2, half, one), BF16),
                pltpu.SemaphoreType.DMA((15,)),
                pltpu.SemaphoreType.DMA((3,)),
                pltpu.SemaphoreType.DMA((3,)),
                pltpu.SemaphoreType.DMA((2,)),
                pltpu.SemaphoreType.DMA((2,)),
                pltpu.SemaphoreType.DMA((3,)),
                pltpu.SemaphoreType.REGULAR((8,)),
            ],
            compiler_params=pltpu.CompilerParams(
                collective_id=0, has_side_effects=True, vmem_limit_bytes=66_000_000
            ),
            name="pyramid",
        )(*operands)
    )


def solution(mesh):
    rows = P(("img", "rows"), None, None)
    return jax.shard_map(
        body,
        mesh=mesh,
        in_specs=(P(None, ("img", "rows"), None),) + (P(),) * 12,
        out_specs=(rows,) * 3,
        check_vma=False,
    )
```

```python
import functools

import jax
import jax.numpy as jnp
from jax import lax
from jax.experimental import pallas as pl
from jax.experimental.pallas import tpu as pltpu
from jax.sharding import PartitionSpec as P

GRID_W = 64
NEAR = 4
F32 = jnp.float32
BF16 = jnp.bfloat16


def dot(a, b):
    return jnp.dot(a, b, preferred_element_type=F32)


def dot_first(a, b):
    return lax.dot_general(a, b, (((0,), (0,)), ((), ())), preferred_element_type=F32)


def iota(shape, dim):
    return lax.broadcasted_iota(jnp.int32, shape, dim)


def one_hot(mask):
    return jnp.where(mask, 1.0, 0.0).astype(BF16)


def kernel(
    shards,
    hidden_hbm,
    cells_hbm,
    w4_hbm,
    b4_hbm,
    w2_hbm,
    b2_hbm,
    w1_hbm,
    b1_hbm,
    u4_hbm,
    c4_hbm,
    u2_hbm,
    c2_hbm,
    join_hbm,
    joined,
    wide,
    same,
    hidden,
    cells,
    w4,
    b4,
    w2,
    b2,
    w1,
    b1,
    u4,
    c4,
    u2,
    c2,
    join,
    in4,
    in2,
    in1,
    send4,
    send2,
    send1,
    edge,
    rim,
    phases,
    mixed,
    load_sem,
    send_sem,
    recv_sem,
    edge_send,
    edge_recv,
    known_sem,
):
    me = lax.axis_index("rows")
    tile = hidden.shape[1]
    half = tile // 2

    def remote(src, dst, send, recv, peer):
        return pltpu.make_async_remote_copy(
            src_ref=src,
            dst_ref=dst,
            send_sem=send,
            recv_sem=recv,
            device_id={"rows": peer},
            device_id_type=pl.DeviceIdType.MESH,
        )

    loads = [
        pltpu.make_async_copy(src, dst, load_sem.at[k])
        for k, (src, dst) in enumerate(
            [
                (cells_hbm, cells),
                (hidden_hbm.at[0], hidden.at[0]),
                (w4_hbm, w4),
                (b4_hbm, b4),
                (hidden_hbm.at[1], hidden.at[1]),
                (w2_hbm, w2),
                (b2_hbm, b2),
                (hidden_hbm.at[2], hidden.at[2]),
                (w1_hbm, w1),
                (b1_hbm, b1),
                (u4_hbm, u4),
                (c4_hbm, c4),
                (join_hbm, join),
                (u2_hbm, u2),
                (c2_hbm, c2),
            ]
        )
    ]
    for load in loads:
        load.start()

    barrier = pltpu.get_barrier_semaphore()
    chips = shards // 2
    z = lax.div(me, 2)
    core = lax.rem(me, 2)
    rounds = chips // 2 // NEAR

    def signal(sem, peer):
        pl.semaphore_signal(
            sem, inc=1, device_id={"rows": peer}, device_id_type=pl.DeviceIdType.MESH
        )

    def around(d):
        return lax.rem(z + d + chips, chips)

    signal(barrier, me + 1 - 2 * core)

    @pl.loop(1, NEAR + 1)
    def _(d):
        for side in (d, -d):
            for other in range(2):
                signal(barrier, 2 * around(side) + other)

    def known(k):
        if k == 0:
            pl.semaphore_wait(barrier, 4 * NEAR + 1)
        else:
            pl.semaphore_wait(known_sem.at[2 * k - 2], 1)
            pl.semaphore_wait(known_sem.at[2 * k - 1], 1)
        if k < rounds - 1:
            signal(known_sem.at[2 * k], 2 * around(NEAR) + core)
            signal(known_sem.at[2 * k + 1], 2 * around(-NEAR) + core)

    loads[0].wait()
    mine = cells[pl.ds(me, 1), :]
    row = iota((tile, tile), 0)
    owner = lax.div(mine, tile) == lax.div(row, 2)
    low = jnp.min(jnp.where(owner, mine, shards * tile), axis=1, keepdims=True)
    outgoing = one_hot(owner & ((mine == low) == (lax.rem(row, 2) == 0)))

    table = cells[...]
    here = lax.div(table, tile) == me
    local = lax.rem(table, tile)
    first = jnp.min(jnp.where(here, local, tile), axis=1, keepdims=True)
    final = jnp.max(jnp.where(here, local, -1), axis=1, keepdims=True)
    twice = one_hot(lax.div(iota((tile, shards), 0), 2) == iota((tile, shards), 1))
    wide_first = dot(twice, jnp.broadcast_to(first, (shards, tile)).astype(F32).astype(BF16))
    wide_last = dot(twice, jnp.broadcast_to(final, (shards, tile)).astype(F32).astype(BF16))
    target = jnp.where(lax.rem(row, 2) == 0, wide_first, wide_last)
    placing = one_hot(target == iota((tile, tile), 1).astype(F32))

    def project(layer, weight, bias):
        value = dot(hidden[layer], weight[...]) + bias[...]
        return dot(outgoing, value.astype(BF16)).astype(BF16)

    sends = (send4, send2, send1)
    arrivals = (in4, in2, in1)

    def put(piece, value):
        sends[piece][...] = value.reshape(shards, 2, value.shape[1])

    def fling(pieces, chip):
        for other in range(2):
            for piece in pieces:
                remote(
                    sends[piece].at[2 * chip + other],
                    arrivals[piece].at[me],
                    send_sem.at[piece],
                    recv_sem.at[piece],
                    2 * chip + other,
                ).start()

    def home(piece):
        pltpu.make_async_copy(
            sends[piece].at[me], arrivals[piece].at[me], recv_sem.at[piece]
        ).start()
        peer = me + 1 - 2 * core
        remote(
            sends[piece].at[peer],
            arrivals[piece].at[me],
            send_sem.at[piece],
            recv_sem.at[piece],
            peer,
        ).start()

    def spanning(pieces, low, high, down=True):
        @pl.loop(0, high - low + 1)
        def _(k):
            d = high - k if down else low + k
            fling(pieces, around(d))

            @pl.when(d < chips // 2)
            def _():
                fling(pieces, around(-d))

    for k in (1, 2, 3):
        loads[k].wait()
    put(0, project(0, w4, b4))
    for k in (4, 5, 6):
        loads[k].wait()
    put(1, project(1, w2, b2))
    for k in (7, 8, 9):
        loads[k].wait()
    put(2, project(2, w1, b1))
    known(0)
    spanning((0, 1, 2), 1, 4)
    known(1)
    spanning((0, 1), 5, 8)
    known(2)
    spanning((0, 1), 9, 12)
    known(3)
    spanning((0,), 13, 16)
    spanning((1, 2), 13, 16)
    for piece in range(3):
        home(piece)

    def collect(piece):
        buffer = arrivals[piece]
        pltpu.make_async_copy(buffer, buffer, recv_sem.at[piece]).wait()
        value = buffer[...].reshape(tile, buffer.shape[2])
        return dot_first(placing, value).astype(BF16)

    tile4 = collect(0)
    edge[...] = tile4
    upper, lower = lax.max(me - 1, 0), lax.min(me + 1, shards - 1)
    to_upper = remote(
        edge.at[pl.ds(0, half)], rim.at[1], edge_send.at[0], edge_recv.at[1], upper
    )
    to_lower = remote(
        edge.at[pl.ds(half, half)], rim.at[0], edge_send.at[1], edge_recv.at[0], lower
    )

    @pl.when(me > 0)
    def _():
        to_upper.start()

    @pl.when(me < shards - 1)
    def _():
        to_lower.start()

    spanning((2,), 5, 12)
    for k in (10, 11, 12):
        loads[k].wait()
    feat = c4.shape[1]
    column = lax.rem(iota((tile, feat), 0), half)

    def spread(value, phase, place):
        place(phase + 1, value)
        if phase == 3:
            rolled = pltpu.roll(value, 1, 0)
            place(0, jnp.where(column[: value.shape[0]] == 0, 0.0, rolled))
        if phase == 0:
            rolled = pltpu.roll(value, value.shape[0] - 1, 0)
            place(5, jnp.where(column[: value.shape[0]] == half - 1, 0.0, rolled))

    for a in range(4):
        for b in range(4):
            at = (a * 4 + b) * feat
            value = dot(tile4, u4[:, at : at + feat]) + c4[...]

            def place(slot, rows, a=a):
                rows = rows.astype(BF16)
                phases[slot, pl.ds((1 + a) * half, half), :] = rows[:half]
                phases[slot, pl.ds((5 + a) * half, half), :] = rows[half:]

            spread(value, b, place)

    @pl.when(me > 0)
    def _():
        to_upper.wait_send()
        to_lower.wait_recv()

    @pl.when(me < shards - 1)
    def _():
        to_lower.wait_send()
        to_upper.wait_recv()

    for side, a, keep, at_row in ((0, 3, me > 0, 0), (1, 0, me < shards - 1, 9)):

        @pl.when(keep)
        def _():
            for b in range(4):
                at = (a * 4 + b) * feat
                value = dot(rim[side], u4[:, at : at + feat]) + c4[...]

                def place(slot, rows):
                    phases[slot, pl.ds(at_row * half, half), :] = rows.astype(BF16)

                spread(value, b, place)

        @pl.when(jnp.logical_not(keep))
        def _():
            for slot in range(6):
                phases[slot, pl.ds(at_row * half, half), :] = jnp.zeros((half, feat), BF16)

    @pl.loop(0, 4)
    def _(phase):
        taps = []
        for a in range(3):
            for b in range(3):
                taps.append(phases[phase + b, pl.ds(a * half, 8 * half), :])
        value = dot(jnp.concatenate(taps, axis=1), join[...])
        mixed[phase] = value.astype(BF16).reshape(8, half, value.shape[1])

    order = iota((4 * half, 4 * half), 0)
    source = iota((4 * half, 4 * half), 1)
    weave4 = one_hot(source == lax.rem(order, 4) * half + lax.div(order, 4))

    @pl.loop(0, 8)
    def _(r):
        columns = mixed[:, r].reshape(4 * half, mixed.shape[3])
        joined[r] = dot(weave4, columns).astype(BF16)

    tile2 = collect(1)
    for k in (13, 14):
        loads[k].wait()
    weave2 = one_hot(
        iota((tile, tile), 1) == lax.rem(row, 2) * half + lax.div(row, 2)
    )
    c_two = c2.shape[1]
    for a in range(2):
        pair = [
            (dot(tile2, u2[:, at : at + c_two]) + c2[...]).astype(BF16)
            for at in ((a * 2) * c_two, (a * 2 + 1) * c_two)
        ]
        for i in range(2):
            both = jnp.concatenate([p[i * half : (i + 1) * half] for p in pair], axis=0)
            wide[2 * i + a] = dot(weave2, both).astype(BF16)

    tile1 = collect(2)
    same[...] = tile1.reshape(2, half, tile1.shape[1])

    for piece in range(3):
        most = sends[piece].at[pl.ds(0, shards - 1)]
        pltpu.make_async_copy(most, most, send_sem.at[piece]).wait()


def keep(joined, wide, same, joined_hbm, up2_hbm, same_hbm, sems):
    pairs = ((joined, joined_hbm), (wide, up2_hbm), (same, same_hbm))
    copies = [pltpu.make_async_copy(a, b, sems.at[k]) for k, (a, b) in enumerate(pairs)]
    for copy in copies:
        copy.start()
    for copy in copies:
        copy.wait()


def body(
    hidden_states,
    cell_of,
    proj_four_weight,
    proj_four_bias,
    proj_two_weight,
    proj_two_bias,
    proj_same_weight,
    proj_same_bias,
    up4_weight,
    up4_bias,
    up2_weight,
    up2_bias,
    join_weight,
):
    shards = lax.axis_size("rows")
    tile = hidden_states.shape[1]
    half = tile // 2
    four, two, one = (
        proj_four_weight.shape[1],
        proj_two_weight.shape[1],
        proj_same_weight.shape[1],
    )
    feat = join_weight.shape[3]
    operands = (
        hidden_states,
        cell_of.reshape(shards, tile),
        proj_four_weight,
        proj_four_bias.reshape(1, -1),
        proj_two_weight,
        proj_two_bias.reshape(1, -1),
        proj_same_weight,
        proj_same_bias.reshape(1, -1),
        up4_weight,
        up4_bias.reshape(1, -1),
        up2_weight,
        up2_bias.reshape(1, -1),
        join_weight.reshape(-1, feat),
    )
    vmem = pltpu.VMEM
    operands = [pltpu.with_memory_space_constraint(o, pltpu.HBM) for o in operands]
    results = pl.pallas_call(
        functools.partial(kernel, shards),
        out_shape=(
            vmem((8, 4 * half, feat), BF16),
            vmem((4, 2 * half, two), BF16),
            vmem((2, half, one), BF16),
        ),
        in_specs=[pl.BlockSpec(memory_space=pltpu.HBM)] * len(operands),
        out_specs=[pl.BlockSpec(memory_space=pltpu.VMEM)] * 3,
        scratch_shapes=[vmem(o.shape, o.dtype) for o in operands]
        + [
            vmem((shards, 2, four), BF16),
            vmem((shards, 2, two), BF16),
            vmem((shards, 2, one), BF16),
            vmem((shards, 2, four), BF16),
            vmem((shards, 2, two), BF16),
            vmem((shards, 2, one), BF16),
            vmem((tile, four), BF16),
            vmem((2, half, four), BF16),
            vmem((6, 10 * half, four), BF16),
            vmem((4, 8, half, feat), BF16),
            pltpu.SemaphoreType.DMA((15,)),
            pltpu.SemaphoreType.DMA((3,)),
            pltpu.SemaphoreType.DMA((3,)),
            pltpu.SemaphoreType.DMA((2,)),
            pltpu.SemaphoreType.DMA((2,)),
            pltpu.SemaphoreType.REGULAR((8,)),
        ],
        compiler_params=pltpu.CompilerParams(
            collective_id=0, has_side_effects=True, vmem_limit_bytes=63_000_000
        ),
        name="pyramid",
    )(*operands)
    return tuple(
        pl.pallas_call(
            keep,
            out_shape=[jax.ShapeDtypeStruct(r.shape, r.dtype) for r in results],
            in_specs=[pl.BlockSpec(memory_space=pltpu.VMEM)] * 3,
            out_specs=[pl.BlockSpec(memory_space=pltpu.HBM)] * 3,
            scratch_shapes=[pltpu.SemaphoreType.DMA((3,))],
            name="keep",
        )(*[pltpu.with_memory_space_constraint(r, pltpu.VMEM) for r in results])
    )


def solution(mesh):
    rows = P(("img", "rows"), None, None)
    return jax.shard_map(
        body,
        mesh=mesh,
        in_specs=(P(None, ("img", "rows"), None),) + (P(),) * 12,
        out_specs=(rows,) * 3,
        check_vma=False,
    )
```

```python
import functools

import jax
import jax.numpy as jnp
from jax import lax
from jax.experimental import pallas as pl
from jax.experimental.pallas import tpu as pltpu
from jax.sharding import PartitionSpec as P

GRID_W = 64
NEAR = 4
F32 = jnp.float32
BF16 = jnp.bfloat16


def dot(a, b):
    return jnp.dot(a, b, preferred_element_type=F32)


def dot_first(a, b):
    return lax.dot_general(a, b, (((0,), (0,)), ((), ())), preferred_element_type=F32)


def iota(shape, dim):
    return lax.broadcasted_iota(jnp.int32, shape, dim)


def one_hot(mask):
    return jnp.where(mask, 1.0, 0.0).astype(BF16)


def kernel(
    shards,
    hidden_hbm,
    cells_hbm,
    w4_hbm,
    b4_hbm,
    w2_hbm,
    b2_hbm,
    w1_hbm,
    b1_hbm,
    u4_hbm,
    c4_hbm,
    u2_hbm,
    c2_hbm,
    join_hbm,
    joined,
    wide,
    same,
    hidden,
    cells,
    w4,
    b4,
    w2,
    b2,
    w1,
    b1,
    u4,
    c4,
    u2,
    c2,
    join,
    in4,
    in2,
    in1,
    send4,
    send2,
    send1,
    edge,
    rim,
    phases,
    mixed,
    load_sem,
    send_sem,
    recv_sem,
    edge_send,
    edge_recv,
    known_sem,
):
    me = lax.axis_index("rows")
    tile = hidden.shape[1]
    half = tile // 2

    def remote(src, dst, send, recv, peer):
        return pltpu.make_async_remote_copy(
            src_ref=src,
            dst_ref=dst,
            send_sem=send,
            recv_sem=recv,
            device_id={"rows": peer},
            device_id_type=pl.DeviceIdType.MESH,
        )

    loads = [
        pltpu.make_async_copy(src, dst, load_sem.at[k])
        for k, (src, dst) in enumerate(
            [
                (cells_hbm, cells),
                (hidden_hbm.at[0], hidden.at[0]),
                (w4_hbm, w4),
                (b4_hbm, b4),
                (hidden_hbm.at[1], hidden.at[1]),
                (w2_hbm, w2),
                (b2_hbm, b2),
                (hidden_hbm.at[2], hidden.at[2]),
                (w1_hbm, w1),
                (b1_hbm, b1),
                (u4_hbm, u4),
                (c4_hbm, c4),
                (join_hbm, join),
                (u2_hbm, u2),
                (c2_hbm, c2),
            ]
        )
    ]
    for load in loads[:10]:
        load.start()

    barrier = pltpu.get_barrier_semaphore()
    chips = shards // 2
    z = lax.div(me, 2)
    core = lax.rem(me, 2)
    rounds = chips // 2 // NEAR

    def signal(sem, peer):
        pl.semaphore_signal(
            sem, inc=1, device_id={"rows": peer}, device_id_type=pl.DeviceIdType.MESH
        )

    def around(d):
        return lax.rem(z + d + chips, chips)

    signal(barrier, me + 1 - 2 * core)

    @pl.loop(1, NEAR + 1)
    def _(d):
        for side in (d, -d):
            for other in range(2):
                signal(barrier, 2 * around(side) + other)

    def known(k):
        if k == 0:
            pl.semaphore_wait(barrier, 4 * NEAR + 1)
        else:
            pl.semaphore_wait(known_sem.at[2 * k - 2], 1)
            pl.semaphore_wait(known_sem.at[2 * k - 1], 1)
        if k < rounds - 1:
            signal(known_sem.at[2 * k], 2 * around(NEAR) + core)
            signal(known_sem.at[2 * k + 1], 2 * around(-NEAR) + core)

    loads[0].wait()
    mine = cells[pl.ds(me, 1), :]
    row = iota((tile, tile), 0)
    owner = lax.div(mine, tile) == lax.div(row, 2)
    low = jnp.min(jnp.where(owner, mine, shards * tile), axis=1, keepdims=True)
    outgoing = one_hot(owner & ((mine == low) == (lax.rem(row, 2) == 0)))

    table = cells[...]
    here = lax.div(table, tile) == me
    local = lax.rem(table, tile)
    first = jnp.min(jnp.where(here, local, tile), axis=1, keepdims=True)
    final = jnp.max(jnp.where(here, local, -1), axis=1, keepdims=True)
    twice = one_hot(lax.div(iota((tile, shards), 0), 2) == iota((tile, shards), 1))
    wide_first = dot(twice, jnp.broadcast_to(first, (shards, tile)).astype(F32).astype(BF16))
    wide_last = dot(twice, jnp.broadcast_to(final, (shards, tile)).astype(F32).astype(BF16))
    target = jnp.where(lax.rem(row, 2) == 0, wide_first, wide_last)
    placing = one_hot(target == iota((tile, tile), 1).astype(F32))

    def project(layer, weight, bias):
        value = dot(hidden[layer], weight[...]) + bias[...]
        return dot(outgoing, value.astype(BF16)).astype(BF16)

    sends = (send4, send2, send1)
    arrivals = (in4, in2, in1)

    def put(piece, value):
        sends[piece][...] = value.reshape(shards, 2, value.shape[1])

    def fling(pieces, chip):
        for other in range(2):
            for piece in pieces:
                remote(
                    sends[piece].at[2 * chip + other],
                    arrivals[piece].at[me],
                    send_sem.at[piece],
                    recv_sem.at[piece],
                    2 * chip + other,
                ).start()

    def home(piece):
        pltpu.make_async_copy(
            sends[piece].at[me], arrivals[piece].at[me], recv_sem.at[piece]
        ).start()
        peer = me + 1 - 2 * core
        remote(
            sends[piece].at[peer],
            arrivals[piece].at[me],
            send_sem.at[piece],
            recv_sem.at[piece],
            peer,
        ).start()

    def spanning(pieces, low, high, down=True):
        @pl.loop(0, high - low + 1)
        def _(k):
            d = high - k if down else low + k
            fling(pieces, around(d))

            @pl.when(d < chips // 2)
            def _():
                fling(pieces, around(-d))

    for k in (1, 2, 3):
        loads[k].wait()
    put(0, project(0, w4, b4))
    for k in (4, 5, 6):
        loads[k].wait()
    put(1, project(1, w2, b2))
    for k in (7, 8, 9):
        loads[k].wait()
    put(2, project(2, w1, b1))
    known(0)
    spanning((0, 1, 2), 1, 4)
    known(1)
    spanning((0, 1), 5, 8)
    known(2)
    spanning((0, 1), 9, 12)
    known(3)
    spanning((0,), 13, 16)
    spanning((1,), 13, 16)
    spanning((2,), 13, 16)
    for load in loads[10:]:
        load.start()
    for piece in range(3):
        home(piece)

    def collect(piece):
        buffer = arrivals[piece]
        pltpu.make_async_copy(buffer, buffer, recv_sem.at[piece]).wait()
        value = buffer[...].reshape(tile, buffer.shape[2])
        return dot_first(placing, value).astype(BF16)

    def sent(piece):
        most = sends[piece].at[pl.ds(0, shards - 1)]
        pltpu.make_async_copy(most, most, send_sem.at[piece]).wait()

    sent(0)
    sent(1)
    spanning((2,), 11, 12)
    tile4 = collect(0)
    edge[...] = tile4
    upper, lower = lax.max(me - 1, 0), lax.min(me + 1, shards - 1)
    to_upper = remote(
        edge.at[pl.ds(0, half)], rim.at[1], edge_send.at[0], edge_recv.at[1], upper
    )
    to_lower = remote(
        edge.at[pl.ds(half, half)], rim.at[0], edge_send.at[1], edge_recv.at[0], lower
    )

    @pl.when(me > 0)
    def _():
        to_upper.start()

    @pl.when(me < shards - 1)
    def _():
        to_lower.start()

    spanning((2,), 5, 10)
    for k in (10, 11, 12):
        loads[k].wait()
    feat = c4.shape[1]
    column = lax.rem(iota((tile, feat), 0), half)

    def spread(value, phase, place):
        place(phase + 1, value)
        if phase == 3:
            rolled = pltpu.roll(value, 1, 0)
            place(0, jnp.where(column[: value.shape[0]] == 0, 0.0, rolled))
        if phase == 0:
            rolled = pltpu.roll(value, value.shape[0] - 1, 0)
            place(5, jnp.where(column[: value.shape[0]] == half - 1, 0.0, rolled))

    for a in range(4):
        for b in range(4):
            at = (a * 4 + b) * feat
            value = dot(tile4, u4[:, at : at + feat]) + c4[...]

            def place(slot, rows, a=a):
                rows = rows.astype(BF16)
                phases[slot, pl.ds((1 + a) * half, half), :] = rows[:half]
                phases[slot, pl.ds((5 + a) * half, half), :] = rows[half:]

            spread(value, b, place)

    @pl.when(me > 0)
    def _():
        to_upper.wait_send()
        to_lower.wait_recv()

    @pl.when(me < shards - 1)
    def _():
        to_lower.wait_send()
        to_upper.wait_recv()

    for side, a, keep, at_row in ((0, 3, me > 0, 0), (1, 0, me < shards - 1, 9)):

        @pl.when(keep)
        def _():
            for b in range(4):
                at = (a * 4 + b) * feat
                value = dot(rim[side], u4[:, at : at + feat]) + c4[...]

                def place(slot, rows):
                    phases[slot, pl.ds(at_row * half, half), :] = rows.astype(BF16)

                spread(value, b, place)

        @pl.when(jnp.logical_not(keep))
        def _():
            for slot in range(6):
                phases[slot, pl.ds(at_row * half, half), :] = jnp.zeros((half, feat), BF16)

    @pl.loop(0, 4)
    def _(phase):
        taps = []
        for a in range(3):
            for b in range(3):
                taps.append(phases[phase + b, pl.ds(a * half, 8 * half), :])
        value = dot(jnp.concatenate(taps, axis=1), join[...])
        mixed[phase] = value.astype(BF16).reshape(8, half, value.shape[1])

    order = iota((4 * half, 4 * half), 0)
    source = iota((4 * half, 4 * half), 1)
    weave4 = one_hot(source == lax.rem(order, 4) * half + lax.div(order, 4))

    @pl.loop(0, 8)
    def _(r):
        columns = mixed[:, r].reshape(4 * half, mixed.shape[3])
        joined[r] = dot(weave4, columns).astype(BF16)

    tile2 = collect(1)
    for k in (13, 14):
        loads[k].wait()
    weave2 = one_hot(
        iota((tile, tile), 1) == lax.rem(row, 2) * half + lax.div(row, 2)
    )
    c_two = c2.shape[1]
    for a in range(2):
        pair = [
            (dot(tile2, u2[:, at : at + c_two]) + c2[...]).astype(BF16)
            for at in ((a * 2) * c_two, (a * 2 + 1) * c_two)
        ]
        for i in range(2):
            both = jnp.concatenate([p[i * half : (i + 1) * half] for p in pair], axis=0)
            wide[2 * i + a] = dot(weave2, both).astype(BF16)

    tile1 = collect(2)
    same[...] = tile1.reshape(2, half, tile1.shape[1])

    sent(2)


def keep(joined, wide, same, joined_hbm, up2_hbm, same_hbm, sems):
    pairs = ((joined, joined_hbm), (wide, up2_hbm), (same, same_hbm))
    rows = [(a.at[r], b.at[r]) for a, b in pairs for r in range(a.shape[0])]
    copies = [pltpu.make_async_copy(a, b, sems.at[k]) for k, (a, b) in enumerate(rows)]
    for copy in copies:
        copy.start()
    for copy in copies:
        copy.wait()


def body(
    hidden_states,
    cell_of,
    proj_four_weight,
    proj_four_bias,
    proj_two_weight,
    proj_two_bias,
    proj_same_weight,
    proj_same_bias,
    up4_weight,
    up4_bias,
    up2_weight,
    up2_bias,
    join_weight,
):
    shards = lax.axis_size("rows")
    tile = hidden_states.shape[1]
    half = tile // 2
    four, two, one = (
        proj_four_weight.shape[1],
        proj_two_weight.shape[1],
        proj_same_weight.shape[1],
    )
    feat = join_weight.shape[3]
    operands = (
        hidden_states,
        cell_of.reshape(shards, tile),
        proj_four_weight,
        proj_four_bias.reshape(1, -1),
        proj_two_weight,
        proj_two_bias.reshape(1, -1),
        proj_same_weight,
        proj_same_bias.reshape(1, -1),
        up4_weight,
        up4_bias.reshape(1, -1),
        up2_weight,
        up2_bias.reshape(1, -1),
        join_weight.reshape(-1, feat),
    )
    vmem = pltpu.VMEM
    operands = [pltpu.with_memory_space_constraint(o, pltpu.HBM) for o in operands]
    results = pl.pallas_call(
        functools.partial(kernel, shards),
        out_shape=(
            vmem((8, 4 * half, feat), BF16),
            vmem((4, 2 * half, two), BF16),
            vmem((2, half, one), BF16),
        ),
        in_specs=[pl.BlockSpec(memory_space=pltpu.HBM)] * len(operands),
        out_specs=[pl.BlockSpec(memory_space=pltpu.VMEM)] * 3,
        scratch_shapes=[vmem(o.shape, o.dtype) for o in operands]
        + [
            vmem((shards, 2, four), BF16),
            vmem((shards, 2, two), BF16),
            vmem((shards, 2, one), BF16),
            vmem((shards, 2, four), BF16),
            vmem((shards, 2, two), BF16),
            vmem((shards, 2, one), BF16),
            vmem((tile, four), BF16),
            vmem((2, half, four), BF16),
            vmem((6, 10 * half, four), BF16),
            vmem((4, 8, half, feat), BF16),
            pltpu.SemaphoreType.DMA((15,)),
            pltpu.SemaphoreType.DMA((3,)),
            pltpu.SemaphoreType.DMA((3,)),
            pltpu.SemaphoreType.DMA((2,)),
            pltpu.SemaphoreType.DMA((2,)),
            pltpu.SemaphoreType.REGULAR((8,)),
        ],
        compiler_params=pltpu.CompilerParams(
            collective_id=0, has_side_effects=True, vmem_limit_bytes=63_000_000
        ),
        name="pyramid",
    )(*operands)
    return tuple(
        pl.pallas_call(
            keep,
            out_shape=[jax.ShapeDtypeStruct(r.shape, r.dtype) for r in results],
            in_specs=[pl.BlockSpec(memory_space=pltpu.VMEM)] * 3,
            out_specs=[pl.BlockSpec(memory_space=pltpu.HBM)] * 3,
            scratch_shapes=[pltpu.SemaphoreType.DMA((sum(r.shape[0] for r in results),))],
            name="keep",
        )(*[pltpu.with_memory_space_constraint(r, pltpu.VMEM) for r in results])
    )


def solution(mesh):
    rows = P(("img", "rows"), None, None)
    return jax.shard_map(
        body,
        mesh=mesh,
        in_specs=(P(None, ("img", "rows"), None),) + (P(),) * 12,
        out_specs=(rows,) * 3,
        check_vma=False,
    )
```
